512 devices in a mesh: lat: 16 (over y, z_hi), lon: 4 (over x), fold: 8 (over z_lo, core).
Axes of the slice: x: 4, y: 4, z: 16 (z_hi: 4, z_lo: 4; z = z_hi * 4 + z_lo), core: 2. Of those that a mesh axis runs over, the one named last changes fastest.
Arguments:
- field: float32 [8, 12, 640, 2560], P('fold', None, 'lat', 'lon'), may hold values from -6 to 6
- row_shift: int32 [8, 12, 640, 2560], P('fold', None, 'lat', 'lon'), may hold values from -4 to 4
- col_shift: int32 [8, 12, 640, 2560], P('fold', None, 'lat', 'lon'), may hold values from -4 to 4
- row_frac: bfloat16 [8, 12, 640, 2560], P('fold', None, 'lat', 'lon'), may hold values from 0 to 1
- col_frac: bfloat16 [8, 12, 640, 2560], P('fold', None, 'lat', 'lon'), may hold values from 0 to 1
- wave_map: int32 [64], replicated, may hold values from 0 to 1279, as said below
- legendre: float32 [64, 640, 1280], P('lon', 'lat'), may hold values from -0.25 to 0.25
- helm_coef: float32 [48], P('fold'), may hold values from 1e-06 to 0.0001
Outputs:
- spectrum: float32 [48, 4, 16, 2560], P('fold', 'lon', 'lat')
The draws below stay inside these ranges and needn't reach their ends.
Inputs may be any that keep to these rules, and one draw needn't show every extreme that they name: `col_shift`: longitude offset of the departure cell. `wave_map`: distinct zonal wavenumbers.
All inputs are finite; a program needn't handle non-finite values.
Results may differ from the reference program's by a relative error of at most 0.0003.
Values sent between devices are 32-bit elements; how exact they have to be, the bound alone decides.
No kernel may reach another device: no remote copies, remote signals or barrier semaphores. Data moves between devices by JAX's collectives and lax.ppermute only.
A program may use at most 64 MiB of HBM per device.

```python
import math
import jax
import jax.numpy as jnp
from jax import lax

LAT_HALF = 640
LON_CELLS = 2560
DEGREES = 1280
SHIFT_MAX = 4
LEVEL_DEV = 12
GROUPS = 8
LEVELS = 48
WAVES_LON = 16
WAVE_SLOTS = 64
N_LON = 4


def draw_wave_map(key, part):
    ordering = jax.random.permutation(key, DEGREES)
    return ordering[:WAVE_SLOTS].astype(jnp.int32)


def plant(result, key, least, largest):
    shape = result.shape
    index_at = [jax.random.randint(jax.random.fold_in(key, axis), (), 0, shape[axis]) for axis in range(len(shape))]
    result = result.at[tuple(index_at)].set(least)
    longest = shape.index(max(shape))
    index_at[longest] = (index_at[longest] + 1) % shape[longest]
    return result.at[tuple(index_at)].set(largest)


def level_of(key, extent, split, smallest, top_value):
    def one(dim, blocks):
        steps = jax.random.uniform(jax.random.fold_in(jax.random.fold_in(key, 6), dim), (blocks,), jnp.float32, smallest / len(split), top_value / len(split))
        return jnp.repeat(jnp.exp(steps), extent[dim] // blocks).reshape((-1,) + (1,) * (len(extent) - dim - 1))

    level = one(*split[0])
    for cut in split[1:]:
        level = level * one(*cut)
    return level


def gaussian(stream_key, dims, scale, bound, pieces=(), held_as=jnp.bfloat16):
    factor_of = level_of(stream_key, dims, pieces, -0.22, 0.18) if pieces else 1.0
    drawn = jax.random.normal(stream_key, dims, jnp.float32) * scale * factor_of
    return jnp.minimum(jnp.maximum(drawn, -bound), bound).astype(held_as)


def setup_inputs(seed: int = 0) -> dict:
    seeds = jax.random.split(jax.random.key(seed), 9)
    return {
        "field": gaussian(seeds[0], (GROUPS, LEVEL_DEV, LAT_HALF, LON_CELLS), 1.0, 6.0, ((0, 8), (2, 16), (3, 4)), jnp.float32),
        "row_shift": plant(jax.random.randint(seeds[1], (GROUPS, LEVEL_DEV, LAT_HALF, LON_CELLS), 0 - SHIFT_MAX, SHIFT_MAX + 1), jax.random.fold_in(seeds[1], 1), 0 - SHIFT_MAX, SHIFT_MAX).astype(jnp.int32),
        "col_shift": plant(jax.random.randint(seeds[2], (GROUPS, LEVEL_DEV, LAT_HALF, LON_CELLS), 0 - SHIFT_MAX, SHIFT_MAX + 1), jax.random.fold_in(seeds[2], 1), 0 - SHIFT_MAX, SHIFT_MAX).astype(jnp.int32),
        "row_frac": jnp.clip(1.0 * jax.random.uniform(seeds[3], (GROUPS, LEVEL_DEV, LAT_HALF, LON_CELLS), jnp.float32) ** level_of(seeds[3], (GROUPS, LEVEL_DEV, LAT_HALF, LON_CELLS), ((0, 8), (2, 16), (3, 4)), -0.2, 0.2), 0.0, 1.0).astype(jnp.bfloat16),
        "col_frac": jnp.clip(1.0 * jax.random.uniform(seeds[4], (GROUPS, LEVEL_DEV, LAT_HALF, LON_CELLS), jnp.float32) ** level_of(seeds[4], (GROUPS, LEVEL_DEV, LAT_HALF, LON_CELLS), ((0, 8), (2, 16), (3, 4)), -0.2, 0.2), 0.0, 1.0).astype(jnp.bfloat16),
        "wave_map": draw_wave_map(jax.random.fold_in(seeds[8], 71), 0),
        "legendre": gaussian(seeds[6], (WAVE_SLOTS, LAT_HALF, DEGREES), LAT_HALF ** -0.5, 0.25, ((0, 4), (1, 16)), jnp.float32),
        "helm_coef": jnp.clip(jnp.exp(math.log(0.0001) - 4.6051702 * jax.random.uniform(seeds[7], (LEVELS,), jnp.float32) ** level_of(seeds[7], (LEVELS,), ((0, 8),), -0.2, 0.2)), 9.999999974752427e-07, 0.0001),
    }


def cubic_weights(fraction):
    return (-fraction * (fraction - 1.0) * (fraction - 2.0) / 6.0, (fraction + 1.0) * (fraction - 1.0) * (fraction - 2.0) / 2.0, -(fraction + 1.0) * fraction * (fraction - 2.0) / 2.0, (fraction + 1.0) * fraction * (fraction - 1.0) / 6.0)

def interpolate(padded, row_shift, col_shift, row_frac, col_frac, margin):
    levels, rows, cols = row_shift.shape
    width = cols + 2 * margin
    flat = padded.reshape(levels, -1)
    row_base = lax.broadcasted_iota(jnp.int32, (levels, rows, cols), 1) + row_shift + (margin - 1)
    col_base = lax.broadcasted_iota(jnp.int32, (levels, rows, cols), 2) + col_shift + (margin - 1)
    start_index = (row_base * width + col_base).reshape(levels, -1).astype(jnp.int32)
    row_weights = cubic_weights(row_frac.astype(jnp.float32).reshape(levels, -1))
    col_weights = cubic_weights(col_frac.astype(jnp.float32).reshape(levels, -1))
    total = jnp.zeros(start_index.shape, jnp.float32)
    for row_step in range(4):
        line = jnp.zeros(start_index.shape, jnp.float32)
        for col_step in range(4):
            taken = jnp.take_along_axis(flat, start_index + (row_step * width + col_step), axis=1)
            line = line + col_weights[col_step] * taken
        total = total + row_weights[row_step] * line
    return total.reshape(levels, rows, cols)

def zonal_table(waves, first_col, count_cols, lon_total):
    col_ids = first_col + lax.iota(jnp.int32, count_cols)
    phase = col_ids[:, None] * waves[None, :] % lon_total
    angle = phase.astype(jnp.float32) * (2.0 * math.pi / lon_total)
    return jnp.stack([jnp.cos(angle), -jnp.sin(angle)], axis=1) / math.sqrt(lon_total)

def reference(field, row_shift, col_shift, row_frac, col_frac, wave_map, legendre, helm_coef):
    margin = SHIFT_MAX + 2
    blocks = GROUPS // 2
    fields = field.reshape(blocks, 2, LEVEL_DEV, LAT_HALF, LON_CELLS)
    opposite = fields[:, ::-1]
    band = opposite[:, :, :, ::-1, :][:, :, :, :margin, :]
    polar = jnp.zeros((blocks, 2, LEVEL_DEV, margin, LON_CELLS), jnp.float32)
    extended = jnp.concatenate([polar, fields, band], axis=3)
    extended = jnp.concatenate([extended[..., -margin:], extended, extended[..., :margin]], axis=4)
    number = blocks * 2 * LEVEL_DEV

    def one_field(items):
        padded, shift_rows, shift_cols, frac_rows, frac_cols = items
        return interpolate(padded[None], shift_rows[None], shift_cols[None], frac_rows[None], frac_cols[None], margin)[0]
    gridded = lax.map(one_field, (extended.reshape(number, LAT_HALF + 2 * margin, LON_CELLS + 2 * margin), row_shift.reshape(number, LAT_HALF, LON_CELLS), col_shift.reshape(number, LAT_HALF, LON_CELLS), row_frac.reshape(number, LAT_HALF, LON_CELLS), col_frac.reshape(number, LAT_HALF, LON_CELLS)))
    gridded = gridded.reshape(blocks, 2, LEVEL_DEV, LAT_HALF, LON_CELLS)
    even = (gridded[:, 0] + gridded[:, 1]).reshape(LEVELS, LAT_HALF, LON_CELLS)
    odd = (gridded[:, 0] - gridded[:, 1]).reshape(LEVELS, LAT_HALF, LON_CELLS)
    table = zonal_table(wave_map, 0, LON_CELLS, LON_CELLS)
    zonal_even = jnp.einsum('lkx,xqs->lsqk', even, table, precision=lax.Precision.HIGHEST)
    zonal_odd = jnp.einsum('lkx,xqs->lsqk', odd, table, precision=lax.Precision.HIGHEST)
    sum_even = jnp.einsum('lsqk,skn->lsqn', zonal_even, legendre, precision=lax.Precision.HIGHEST)
    sum_odd = jnp.einsum('lsqk,skn->lsqn', zonal_odd, legendre, precision=lax.Precision.HIGHEST)
    degrees = jnp.arange(DEGREES, dtype=jnp.int32)
    parity = (wave_map[:, None] + degrees[None, :]) % 2 == 0
    keep = (degrees[None, :] >= wave_map[:, None]).astype(jnp.float32)
    legendre_sum = jnp.where(parity[None, :, None, :], sum_even, sum_odd) * keep[None, :, None, :]
    degree_float = degrees.astype(jnp.float32)
    damping = 1.0 + helm_coef[:, None, None, None] * (degree_float * (degree_float + 1.0))[None, None, None, :]
    spectrum = legendre_sum / damping
    return spectrum.reshape(LEVELS, N_LON, WAVES_LON, 2 * DEGREES)
```

```python
import math

import jax
import jax.numpy as jnp
from jax import lax
from jax.experimental import pallas as pl
from jax.experimental.pallas import tpu as pltpu
from jax.sharding import Mesh, PartitionSpec as P

LEVELS = 12
HALF = 6
ROWS = 40
COLS = 640
TILES = 5
DEG = 1280
LON_TOTAL = 2560
WIN = 107
NWIN = 6
KDIM = NWIN * 128
VM = pltpu.CompilerParams(vmem_limit_bytes=48 * 1024 * 1024)
LAT = ("y", "zh")
LATF = ("y", "zh", "zl", "core")


def lane_iota():
    return lax.broadcasted_iota(jnp.int32, (8, 128), 1)


def roll(x, shift):
    shift %= 128
    return pltpu.roll(x, shift, 1) if shift else x


def vmem():
    return pl.BlockSpec(memory_space=pltpu.VMEM)


def smem():
    return pl.BlockSpec(memory_space=pltpu.SMEM)


def f32(*dims):
    return jax.ShapeDtypeStruct(dims, jnp.float32)


def lat_index():
    return lax.axis_index("y") * 4 + lax.axis_index("zh")


def edges_kernel(field, lat_even, lat_odd, lon_even, lon_odd):
    lat = lat_index()
    odd = lat % 2
    for j in range(6):
        at_even = jnp.where(odd == 0, 34 + j, j)
        at_odd = jnp.where(odd == 0, j, jnp.where(lat == 15, 39 - j, 34 + j))
        for l in range(LEVELS):
            lat_even[pl.ds(6 * l + j, 1), :] = field[0, l, pl.ds(at_even, 1), :]
            lat_odd[pl.ds(6 * l + j, 1), :] = field[0, l, pl.ds(at_odd, 1), :]
    lane = lane_iota()
    lon_par = lax.axis_index("lon") % 2
    for rt in range(TILES):
        rows = slice(8 * rt, 8 * rt + 8)
        left = jnp.zeros((8, 128), jnp.float32)
        right = jnp.zeros((8, 128), jnp.float32)
        for l in range(LEVELS):
            here = (lane >= 8 * l) & (lane < 8 * l + 6)
            left = jnp.where(here, roll(field[0, l, rows, 0:128], 8 * l), left)
            right = jnp.where(here, roll(field[0, l, rows, 512:640], 8 * l - 122), right)
        lon_even[rows, :] = jnp.where(lon_par == 0, right, left)
        lon_odd[rows, :] = jnp.where(lon_par == 0, left, right)


def corner_kernel(lon_even, lon_odd, to_even, to_odd):
    lat = lat_index()
    odd = lat % 2
    for r in range(8):
        at_even = jnp.where(odd == 0, 32 + r, r)
        at_odd = jnp.where(odd == 0, r, jnp.where(lat == 15, 39 - r, 32 + r))
        for k, ref in enumerate((lon_even, lon_odd)):
            to_even[pl.ds(8 * k + r, 1), :] = ref[pl.ds(at_even, 1), :]
            to_odd[pl.ds(8 * k + r, 1), :] = ref[pl.ds(at_odd, 1), :]


def cubic(t):
    down = t - 1.0
    two = t - 2.0
    up = t + 1.0
    inner = t * down
    outer = up * two
    return (
        inner * two * (-1.0 / 6.0),
        outer * down * 0.5,
        outer * t * (-0.5),
        up * inner * (1.0 / 6.0),
    )


def window(tiles, start, lane):
    first, off = divmod(start, 128)
    x = tiles[first]
    if off:
        if first + 1 < len(tiles):
            x = jnp.where(lane >= off, x, tiles[first + 1])
        x = roll(x, -off)
    return x


def take(x, index):
    return jnp.take_along_axis(x, index, axis=1, mode="promise_in_bounds")


def put_windows(win, row, tiles, lane):
    for w in range(NWIN):
        win[w, row : row + 8, :] = window(tiles, WIN * w + 123, lane)


def lon_sides(lon_even, lon_odd, rows, lon_par):
    even = lon_even[rows, :]
    odd = lon_odd[rows, :]
    return jnp.where(lon_par == 0, odd, even), jnp.where(lon_par == 0, even, odd)


def dyn_roll(x, shift):
    return pltpu.roll(x, shift, 1)


def tile_points(win, at, w, shift_row, shift_col, frac_row, frac_col, lane):
    def cut(ref_tiles):
        return window(ref_tiles, WIN * w, lane)

    rs = cut(shift_row)
    cs = cut(shift_col)
    wr = cubic(cut(frac_row))
    wc = cubic(cut(frac_col))
    first = jnp.minimum(cs + (lane + 4), 124)
    index = [first, first + 1, first + 2, first + 3]
    line = []
    for k in range(12):
        src = win[w, at + k - 5 : at + k + 3, :]
        acc = wc[0] * take(src, index[0])
        for b in range(1, 4):
            acc = acc + wc[b] * take(src, index[b])
        line.append(acc)
    u = rs + 4
    m = u >= 5
    line = [jnp.where(m, line[k + 5], line[k]) for k in range(7)] + [line[7]]
    u = jnp.where(m, u - 5, u)
    m = u >= 3
    line = [jnp.where(m, line[k + 3], line[k]) for k in range(5)] + [line[5]]
    u = jnp.where(m, u - 3, u)
    m = u >= 2
    line = [jnp.where(m, line[k + 2], line[k]) for k in range(4)] + [line[4]]
    m = u == 1
    line = [jnp.where(m, line[k + 1], line[k]) for k in range(4)]
    total = wr[0] * line[0]
    for a in range(1, 4):
        total = total + wr[a] * line[a]
    return total


def lane_tiles(ref, l, rt):
    x = ref[0, l, pl.ds(8 * rt, 8), :]
    if x.dtype == jnp.bfloat16:
        x = x.astype(jnp.float32)
    return [x[:, 128 * t : 128 * t + 128] for t in range(TILES)]


def main_rows(win, field, lon_even, lon_odd, l, row_tiles, lon_par, lane):
    for rt in row_tiles:
        left, right = lon_sides(lon_even, lon_odd, slice(8 * rt, 8 * rt + 8), lon_par)
        tiles = [dyn_roll(left, (250 - 8 * l) % 128)] + lane_tiles(field, l, rt) + [dyn_roll(right, (128 - 8 * l) % 128)]
        put_windows(win, 8 + 8 * rt, tiles, lane)


def split(x):
    hi = x.astype(jnp.bfloat16)
    return hi, (x - hi.astype(jnp.float32)).astype(jnp.bfloat16)


def dot(a, b):
    return jnp.dot(a, b, preferred_element_type=jnp.float32)


def zonal(grid, table):
    hi, lo = split(grid)
    t_hi, t_lo = split(table)
    return dot(hi, t_hi) + (dot(lo, t_hi) + dot(hi, t_lo))


def points_of(l, rt, win, row_shift, col_shift, row_frac, col_frac, lane, put):
    params = [lane_tiles(r, l, rt) for r in (row_shift, col_shift, row_frac, col_frac)]
    for w in range(NWIN):
        put(w, tile_points(win, 8 + 8 * rt, w, *params, lane))


def inner_kernel(field, row_shift, col_shift, row_frac, col_frac, lon_even, lon_odd, table, out, win, grid):
    lane = lane_iota()
    lon_par = lax.axis_index("lon") % 2

    def level(l, carry):
        main_rows(win, field, lon_even, lon_odd, l, range(TILES), lon_par, lane)
        for i in range(3):

            def put(w, x, i=i):
                grid[pl.ds(24 * l + 8 * i, 8), 128 * w : 128 * w + 128] = x

            points_of(l, i + 1, win, row_shift, col_shift, row_frac, col_frac, lane, put)
        return carry

    lax.fori_loop(0, LEVELS, level, 0)
    out[...] = zonal(grid[...], table[...])


def transposed_groups(block, lane):
    group = lane // 8
    for k in (8, 4, 2, 1):
        bit = (group & k) != 0
        new = list(block)
        for i in range(16):
            if not i & k:
                a, b = block[i], block[i + k]
                new[i] = jnp.where(bit, roll(b, 8 * k), a)
                new[i + k] = jnp.where(bit, b, roll(a, -8 * k))
        block = new
    return block


def outer_kernel(
    field,
    row_shift,
    col_shift,
    row_frac,
    col_frac,
    lon_even,
    lon_odd,
    lat_even,
    lat_odd,
    corner_even,
    corner_odd,
    table,
    inner,
    out,
    win,
    grid,
    zon,
    halo,
    side,
):
    lane = lane_iota()
    lon_par = lax.axis_index("lon") % 2
    lat_odd_place = lat_index() % 2

    def place(before, after, corner_before, corner_after):
        for l in range(LEVELS):
            halo[0, l, 2:8, :] = before[6 * l : 6 * l + 6, :]
            halo[1, l, 0:6, :] = after[6 * l : 6 * l + 6, :]
        side[0] = corner_before[...]
        side[1] = corner_after[...]

    for l in range(LEVELS):
        halo[0, l, 0:2, :] = jnp.zeros((2, COLS), jnp.float32)
        halo[1, l, 6:8, :] = jnp.zeros((2, COLS), jnp.float32)

    @pl.when(lat_odd_place == 0)
    def _():
        place(lat_odd, lat_even, corner_odd, corner_even)

    @pl.when(lat_odd_place == 1)
    def _():
        place(lat_even, lat_odd, corner_even, corner_odd)

    def level(l, carry):
        main_rows(win, field, lon_even, lon_odd, l, (0, 1, 3, 4), lon_par, lane)
        for k, row in ((0, 0), (1, 48)):
            even = side[k, 0:8, :]
            odd = side[k, 8:16, :]
            left = jnp.where(lon_par == 0, odd, even)
            right = jnp.where(lon_par == 0, even, odd)
            x = halo[k, l]
            tiles = [x[:, 128 * t : 128 * t + 128] for t in range(TILES)]
            tiles = [dyn_roll(left, (250 - 8 * l) % 128)] + tiles + [dyn_roll(right, (128 - 8 * l) % 128)]
            put_windows(win, row, tiles, lane)
        for i, rt in enumerate((0, 4)):

            def put(w, x, i=i):
                grid[pl.ds(16 * l + 8 * i, 8), 128 * w : 128 * w + 128] = x

            points_of(l, rt, win, row_shift, col_shift, row_frac, col_frac, lane, put)
        return carry

    lax.fori_loop(0, LEVELS, level, 0)
    zon[...] = zonal(grid[...], table[...])
    for core in range(2):
        for v in range(2):
            block = []
            for p in range(16 * v, 16 * v + 16):
                rt, l = divmod(min(p, 29), HALF)
                l += HALF * core
                if rt in (0, 4):
                    at = 16 * l + (8 if rt else 0)
                    block.append(zon[at : at + 8, :])
                else:
                    at = 24 * l + 8 * (rt - 1)
                    block.append(inner[at : at + 8, :])
            block = transposed_groups(block, lane)
            for d in range(16):
                lon, y = divmod(d, 4)
                out[y * 8 + lon * 2 + core, 8 * v : 8 * v + 8, :] = block[d]


def legendre_kernel(wave_map, arrived, legendre, from_1, from_2, from_3, out, lhs):
    lane = lane_iota()
    place = lax.axis_index("y")
    pieces = []
    for v in range(2):
        half = {}
        for y in range(4):
            sums = []
            for core in range(2):
                x = arrived[(place ^ y) * 8 + core, 8 * v : 8 * v + 8, :]
                for lon in range(1, 4):
                    x = x + arrived[(place ^ y) * 8 + lon * 2 + core, 8 * v : 8 * v + 8, :]
                sums.append(x)
            half[0, y] = sums[0] + sums[1]
            half[1, y] = sums[0] - sums[1]
        pieces += [half[e, y] for e in range(2) for y in range(4)]
    turned = jnp.concatenate(pieces, axis=0).T
    lhs[...] = jnp.zeros(lhs.shape, jnp.float32)
    for e in range(2):
        for l in range(HALF):
            first = jnp.zeros((8, 128), jnp.float32)
            last = jnp.zeros((8, 128), jnp.float32)
            for rt in range(TILES):
                v, p = divmod(rt * HALF + l, 16)
                x = turned[8 * p : 8 * p + 8, :]
                x = roll(x, 32 * (rt % 4) - (64 * v + 32 * e))
                here = (lane >= 32 * (rt % 4)) & (lane < 32 * (rt % 4) + 32)
                if rt < 4:
                    first = jnp.where(here, x, first)
                else:
                    last = jnp.where(here, x, last)
            for s in range(4):
                lhs[s, 16 * e + 2 * l : 16 * e + 2 * l + 2, 0:128] = first[2 * s : 2 * s + 2, :]
                lhs[s, 16 * e + 2 * l : 16 * e + 2 * l + 2, 128:256] = last[2 * s : 2 * s + 2, :]
    slot = lax.axis_index("lon") * 16 + lax.axis_index("y") * 4
    degree = lax.broadcasted_iota(jnp.int32, (16, DEG), 1)
    low = lax.broadcasted_iota(jnp.int32, (8, 128), 0) < 4
    for s in range(4):
        wave = wave_map[slot + s]
        a_hi, a_lo = split(lhs[s][:, 0:160])
        rows = []
        for rt in range(TILES):
            at = slice(40 * s + 8 * rt, 40 * s + 8 * rt + 8)
            rows += [legendre[place, at, :], from_1[at, :], from_2[at, :], from_3[at, :]]
        b_hi, b_lo = split(jnp.concatenate(rows, axis=0))
        sums = dot(a_hi, b_hi) + (dot(a_lo, b_hi) + dot(a_hi, b_lo))
        picked = jnp.where((degree + wave) % 2 == 0, sums[0:16], sums[16:32])
        picked = jnp.where(degree >= wave, picked, 0.0)
        for j in range(10):
            out[s, 8 * j : 8 * j + 8, :] = picked[0:8, 128 * j : 128 * j + 128]
        for j in range(0, 10, 2):
            a = picked[8:16, 128 * j : 128 * j + 128]
            b = picked[8:16, 128 * j + 128 : 128 * j + 256]
            out[s, 80 + 4 * j : 88 + 4 * j, :] = jnp.where(low, a, pltpu.roll(b, 4, 0))


def finish_kernel(helm, parts, out):
    total = parts[0] + parts[1] + (parts[2] + parts[3])
    row = lax.broadcasted_iota(jnp.int32, (8, 128), 0)
    lane = lane_iota()

    def damped(x, first, degree):
        coef = jnp.zeros((8, 128), jnp.float32)
        for i in range(4):
            coef = jnp.where(row // 2 == i, helm[(first + i) % HALF if first + i < HALF else 4 + i % 2], coef)
        return x / (1.0 + coef * (degree * (degree + 1.0)))

    for j in range(10):
        degree = (lane + 128 * j).astype(jnp.float32)
        x = damped(total[8 * j : 8 * j + 8, :], 0, degree)
        for i in range(8):
            l, q = divmod(i, 2)
            out[l, 0, 0, q * DEG + 128 * j : q * DEG + 128 * j + 128] = x[i, :]
    for j in range(0, 10, 2):
        degree = (lane + 128 * j + jnp.where(row < 4, 0, 128)).astype(jnp.float32)
        x = damped(total[80 + 4 * j : 88 + 4 * j, :], 4, degree)
        for i in range(8):
            l, q = divmod(i % 4, 2)
            at = q * DEG + 128 * (j + i // 4)
            out[4 + l, 0, 0, at : at + 128] = x[i, :]


def zonal_table(wave_map):
    k = lax.broadcasted_iota(jnp.int32, (KDIM, 128), 0)
    lane = lax.broadcasted_iota(jnp.int32, (KDIM, 128), 1)
    i = k % 128
    col = k // 128 * WIN + i
    valid = (i < WIN) & (col < COLS)
    phase = (col + lax.axis_index("lon") * COLS) * jnp.repeat(wave_map, 2)[None, :] % LON_TOTAL
    phase = (phase + (lane % 2) * (LON_TOTAL // 4)) % LON_TOTAL
    angle = phase.astype(jnp.float32) * (2.0 * math.pi / LON_TOTAL)
    return jnp.where(valid, jnp.cos(angle) / math.sqrt(LON_TOTAL), 0.0)


def lon_pairs(odd):
    return [r for i in range(odd, 4, 2) for r in ((i, (i + 1) % 4), ((i + 1) % 4, i))]


def lat_pairs(odd):
    route = []
    for i in range(odd, 15, 2):
        for f in range(8):
            low, high = i * 8 + f, (i + 1) * 8 + f
            route += [(low, high), (high, low)]
    if odd:
        for f in range(8):
            route.append((15 * 8 + f, 15 * 8 + (f ^ 1)))
    return route


def call(kernel, outs, count, scratch=(), smem_first=0):
    specs = [smem()] * smem_first + [vmem()] * (count - smem_first)
    return pl.pallas_call(
        kernel,
        out_shape=outs,
        in_specs=specs,
        out_specs=jax.tree.map(lambda _: vmem(), outs),
        scratch_shapes=list(scratch),
        compiler_params=VM,
    )


def stages(field, row_shift, col_shift, row_frac, col_frac, wave_map, legendre, helm_coef):
    grid_args = (field, row_shift, col_shift, row_frac, col_frac)
    lat_e, lat_o, lon_e, lon_o = call(edges_kernel, (f32(72, COLS), f32(72, COLS), f32(ROWS, 128), f32(ROWS, 128)), 1)(field)
    lat_e = lax.ppermute(lat_e, LATF, lat_pairs(0))
    lat_o = lax.ppermute(lat_o, LATF, lat_pairs(1))
    lon_e = lax.ppermute(lon_e, "lon", lon_pairs(0))
    lon_o = lax.ppermute(lon_o, "lon", lon_pairs(1))
    cor_e, cor_o = call(corner_kernel, (f32(16, 128), f32(16, 128)), 2)(lon_e, lon_o)
    cor_e = lax.ppermute(cor_e, LATF, lat_pairs(0))
    cor_o = lax.ppermute(cor_o, LATF, lat_pairs(1))
    legendre = legendre.reshape(4, 4 * ROWS, DEG)
    place = lax.axis_index("y")
    arrived_rows = [
        lax.ppermute(lax.dynamic_index_in_dim(legendre, place ^ d, 0, keepdims=False), "y", [(i, i ^ d) for i in range(4)])
        for d in (1, 2, 3)
    ]
    table = zonal_table(wave_map)
    win = pltpu.VMEM((NWIN, 56, 128), jnp.float32)
    inner = call(inner_kernel, f32(LEVELS * 24, 128), 8, (win, pltpu.VMEM((LEVELS * 24, KDIM), jnp.float32)))(
        *grid_args, lon_e, lon_o, table
    )
    sent = call(
        outer_kernel,
        f32(32, 16, 128),
        13,
        (
            win,
            pltpu.VMEM((LEVELS * 16, KDIM), jnp.float32),
            pltpu.VMEM((LEVELS * 16, 128), jnp.float32),
            pltpu.VMEM((2, LEVELS, 8, COLS), jnp.float32),
            pltpu.VMEM((2, 16, 128), jnp.float32),
        ),
    )(*grid_args, lon_e, lon_o, lat_e, lat_o, cor_e, cor_o, table, inner)
    arrived = lax.all_to_all(sent, ("y", "lon", "core"), 0, 0, tiled=True)
    parts = call(legendre_kernel, f32(4, 120, 128), 6, (pltpu.VMEM((4, 32, 256), jnp.float32),), 1)(
        wave_map, arrived, legendre, *arrived_rows
    )
    parts = lax.all_to_all(parts, "zh", 0, 0, tiled=True)
    return call(finish_kernel, f32(HALF, 1, 1, 2 * DEG), 2, (), 1)(helm_coef, parts)


def solution(mesh):
    fine = Mesh(mesh.devices.reshape(4, 4, 4, 4, 2), ("y", "zh", "lon", "zl", "core"))
    fold = ("zl", "core")
    block = P(fold, None, LAT, "lon")
    in_specs = (block, block, block, block, block, P(), P("lon", LAT, None), P(fold))
    return jax.shard_map(stages, mesh=fine, in_specs=in_specs, out_specs=P(fold, "lon", LAT, None), check_vma=False)
```

```python
import math

import jax
import jax.numpy as jnp
from jax import lax
from jax.experimental import pallas as pl
from jax.experimental.pallas import tpu as pltpu
from jax.sharding import Mesh, PartitionSpec as P

LEVELS = 12
HALF = 6
ROWS = 40
COLS = 640
TILES = 5
DEG = 1280
LON_TOTAL = 2560
VM = pltpu.CompilerParams(vmem_limit_bytes=48 * 1024 * 1024)
LAT = ("y", "zh")
LATF = ("y", "zh", "zl", "core")


def lane_iota():
    return lax.broadcasted_iota(jnp.int32, (8, 128), 1)


def roll(x, shift):
    shift %= 128
    return pltpu.roll(x, shift, 1) if shift else x


def vmem():
    return pl.BlockSpec(memory_space=pltpu.VMEM)


def smem():
    return pl.BlockSpec(memory_space=pltpu.SMEM)


def f32(*dims):
    return jax.ShapeDtypeStruct(dims, jnp.float32)


def lat_index():
    return lax.axis_index("y") * 4 + lax.axis_index("zh")


def edges_kernel(field, lat_even, lat_odd, lon_even, lon_odd):
    lane = lane_iota()
    lon_par = lax.axis_index("lon") % 2
    for rt in range(TILES):
        rows = slice(8 * rt, 8 * rt + 8)
        left = jnp.zeros((8, 128), jnp.float32)
        right = jnp.zeros((8, 128), jnp.float32)
        for l in range(LEVELS):
            here = (lane >= 8 * l) & (lane < 8 * l + 6)
            left = jnp.where(here, roll(field[0, l, rows, 0:128], 8 * l), left)
            right = jnp.where(here, roll(field[0, l, rows, 512:640], 8 * l - 122), right)
        lon_even[rows, :] = jnp.where(lon_par == 0, right, left)
        lon_odd[rows, :] = jnp.where(lon_par == 0, left, right)
    for j, at_even, at_odd in edge_rows():
        for l in range(LEVELS):
            lat_even[pl.ds(6 * l + j, 1), :] = field[0, l, pl.ds(at_even, 1), :]
            lat_odd[pl.ds(6 * l + j, 1), :] = field[0, l, pl.ds(at_odd, 1), :]
    lat_even[72:80, :] = jnp.zeros((8, COLS), jnp.float32)
    lat_odd[72:80, :] = jnp.zeros((8, COLS), jnp.float32)


def edge_rows():
    lat = lat_index()
    odd = lat % 2
    for j in range(6):
        at_even = jnp.where(odd == 0, 34 + j, j)
        at_odd = jnp.where(odd == 0, j, jnp.where(lat == 15, 39 - j, 34 + j))
        yield j, at_even, at_odd


def corner_kernel(lon_even, lon_odd, _even, _odd, lat_even, lat_odd):
    for j, at_even, at_odd in edge_rows():
        for k, ref in enumerate((lon_even, lon_odd)):
            lat_even[72 + j : 73 + j, 128 * k : 128 * k + 128] = ref[pl.ds(at_even, 1), :]
            lat_odd[72 + j : 73 + j, 128 * k : 128 * k + 128] = ref[pl.ds(at_odd, 1), :]
    lat_even[78:80, :] = jnp.zeros((2, COLS), jnp.float32)
    lat_odd[78:80, :] = jnp.zeros((2, COLS), jnp.float32)
    for ref in (lat_even, lat_odd):
        ref[72:78, 256:COLS] = jnp.zeros((6, COLS - 256), jnp.float32)


def cubic(t):
    down = t - 1.0
    two = t - 2.0
    up = t + 1.0
    inner = t * down
    outer = up * two
    return (
        inner * two * (-1.0 / 6.0),
        outer * down * 0.5,
        outer * t * (-0.5),
        up * inner * (1.0 / 6.0),
    )


def put_shifted(sh, row, tiles, lane):
    for t in range(TILES):
        for k in range(12):
            off = k - 5
            x = tiles[t + 1]
            if off > 0:
                x = roll(jnp.where(lane >= off, x, tiles[t + 2]), -off)
            elif off < 0:
                x = roll(jnp.where(lane < 128 + off, x, tiles[t]), -off)
            sh[k * TILES + t, row : row + 8, :] = x


def lon_sides(lon_even, lon_odd, rows, lon_par):
    even = lon_even[rows, :]
    odd = lon_odd[rows, :]
    return jnp.where(lon_par == 0, odd, even), jnp.where(lon_par == 0, even, odd)


def dyn_roll(x, shift):
    return pltpu.roll(x, shift, 1)


def spread(shift, weights):
    here = [shift == k for k in range(-4, 5)]
    placed = []
    for k in range(12):
        value = None
        for a in range(4):
            if 0 <= k - a < 9:
                value = jnp.where(here[k - a], weights[a], 0.0 if value is None else value)
        placed.append(value)
    return placed


def tile_points(sh, at, t, rs, cs, row_frac, col_frac):
    wc = spread(cs, cubic(col_frac))
    line = []
    for k in range(12):
        acc = None
        for o in range(12):
            got = wc[o] * sh[o * TILES + t, at + k - 5 : at + k + 3, :]
            acc = got if acc is None else acc + got
        line.append(acc)
    wr = cubic(row_frac)
    u = rs + 4
    m = u >= 5
    line = [jnp.where(m, line[k + 5], line[k]) for k in range(7)] + [line[7]]
    u = jnp.where(m, u - 5, u)
    m = u >= 3
    line = [jnp.where(m, line[k + 3], line[k]) for k in range(5)] + [line[5]]
    u = jnp.where(m, u - 3, u)
    m = u >= 2
    line = [jnp.where(m, line[k + 2], line[k]) for k in range(4)] + [line[4]]
    m = u == 1
    line = [jnp.where(m, line[k + 1], line[k]) for k in range(4)]
    total = wr[0] * line[0]
    for a in range(1, 4):
        total = total + wr[a] * line[a]
    return total


def lane_tiles(ref, l, rt):
    x = ref[0, l, pl.ds(8 * rt, 8), :]
    if x.dtype == jnp.bfloat16:
        x = x.astype(jnp.float32)
    return [x[:, 128 * t : 128 * t + 128] for t in range(TILES)]


def main_rows(win, field, lon_even, lon_odd, l, row_tiles, lon_par, lane):
    for rt in row_tiles:
        left, right = lon_sides(lon_even, lon_odd, slice(8 * rt, 8 * rt + 8), lon_par)
        tiles = [dyn_roll(left, (250 - 8 * l) % 128)] + lane_tiles(field, l, rt) + [dyn_roll(right, (128 - 8 * l) % 128)]
        put_shifted(win, 8 + 8 * rt, tiles, lane)


def split(x):
    hi = x.astype(jnp.bfloat16)
    return hi, (x - hi.astype(jnp.float32)).astype(jnp.bfloat16)


def dot(a, b):
    return jnp.dot(a, b, preferred_element_type=jnp.float32)


def zonal(grid, table):
    hi, lo = split(grid)
    t_hi, t_lo = split(table)
    return dot(hi, t_hi) + (dot(lo, t_hi) + dot(hi, t_lo))


def points_of(l, rt, win, row_shift, col_shift, row_frac, col_frac, put):
    params = [lane_tiles(r, l, rt) for r in (row_shift, col_shift, row_frac, col_frac)]
    for t in range(TILES):
        put(t, tile_points(win, 8 + 8 * rt, t, *[p[t] for p in params]))


def inner_kernel(field, row_shift, col_shift, row_frac, col_frac, lon_even, lon_odd, table, out, win, grid):
    lane = lane_iota()
    lon_par = lax.axis_index("lon") % 2

    def level(l, carry):
        main_rows(win, field, lon_even, lon_odd, l, range(TILES), lon_par, lane)
        for i in range(3):

            def put(w, x, i=i):
                grid[pl.ds(24 * l + 8 * i, 8), 128 * w : 128 * w + 128] = x

            points_of(l, i + 1, win, row_shift, col_shift, row_frac, col_frac, put)
        return carry

    lax.fori_loop(0, LEVELS, level, 0)
    out[...] = zonal(grid[...], table[...])


def transposed_groups(block, lane):
    group = lane // 8
    for k in (8, 4, 2, 1):
        bit = (group & k) != 0
        new = list(block)
        for i in range(16):
            if not i & k:
                a, b = block[i], block[i + k]
                new[i] = jnp.where(bit, roll(b, 8 * k), a)
                new[i + k] = jnp.where(bit, b, roll(a, -8 * k))
        block = new
    return block


def outer_kernel(
    field,
    row_shift,
    col_shift,
    row_frac,
    col_frac,
    lon_even,
    lon_odd,
    lat_even,
    lat_odd,
    table,
    inner,
    out,
    win,
    grid,
    zon,
    halo,
    side,
):
    lane = lane_iota()
    lon_par = lax.axis_index("lon") % 2
    lat_odd_place = lat_index() % 2

    def place(before, after):
        for l in range(LEVELS):
            halo[0, l, 2:8, :] = before[6 * l : 6 * l + 6, :]
            halo[1, l, 0:6, :] = after[6 * l : 6 * l + 6, :]
        for k in range(2):
            side[0, k, 2:8, :] = before[72:78, 128 * k : 128 * k + 128]
            side[1, k, 0:6, :] = after[72:78, 128 * k : 128 * k + 128]

    for l in range(LEVELS):
        halo[0, l, 0:2, :] = jnp.zeros((2, COLS), jnp.float32)
        halo[1, l, 6:8, :] = jnp.zeros((2, COLS), jnp.float32)
    for k in range(2):
        side[0, k, 0:2, :] = jnp.zeros((2, 128), jnp.float32)
        side[1, k, 6:8, :] = jnp.zeros((2, 128), jnp.float32)

    @pl.when(lat_odd_place == 0)
    def _():
        place(lat_odd, lat_even)

    @pl.when(lat_odd_place == 1)
    def _():
        place(lat_even, lat_odd)

    def level(l, carry):
        main_rows(win, field, lon_even, lon_odd, l, (0, 1, 3, 4), lon_par, lane)
        for k, row in ((0, 0), (1, 48)):
            even = side[k, 0]
            odd = side[k, 1]
            left = jnp.where(lon_par == 0, odd, even)
            right = jnp.where(lon_par == 0, even, odd)
            x = halo[k, l]
            tiles = [x[:, 128 * t : 128 * t + 128] for t in range(TILES)]
            tiles = [dyn_roll(left, (250 - 8 * l) % 128)] + tiles + [dyn_roll(right, (128 - 8 * l) % 128)]
            put_shifted(win, row, tiles, lane)
        for i, rt in enumerate((0, 4)):

            def put(w, x, i=i):
                grid[pl.ds(16 * l + 8 * i, 8), 128 * w : 128 * w + 128] = x

            points_of(l, rt, win, row_shift, col_shift, row_frac, col_frac, put)
        return carry

    lax.fori_loop(0, LEVELS, level, 0)
    zon[...] = zonal(grid[...], table[...])
    for core in range(2):
        for v in range(2):
            block = []
            for p in range(16 * v, 16 * v + 16):
                rt, l = divmod(min(p, 29), HALF)
                l += HALF * core
                if rt in (0, 4):
                    at = 16 * l + (8 if rt else 0)
                    block.append(zon[at : at + 8, :])
                else:
                    at = 24 * l + 8 * (rt - 1)
                    block.append(inner[at : at + 8, :])
            block = transposed_groups(block, lane)
            for d in range(16):
                lon, y = divmod(d, 4)
                out[y * 8 + lon * 2 + core, 8 * v : 8 * v + 8, :] = block[d]


def legendre_kernel(wave_map, arrived, legendre, from_1, from_2, from_3, out, lhs):
    lane = lane_iota()
    place = lax.axis_index("y")
    pieces = []
    for v in range(2):
        half = {}
        for y in range(4):
            sums = []
            for core in range(2):
                x = arrived[(place ^ y) * 8 + core, 8 * v : 8 * v + 8, :]
                for lon in range(1, 4):
                    x = x + arrived[(place ^ y) * 8 + lon * 2 + core, 8 * v : 8 * v + 8, :]
                sums.append(x)
            half[0, y] = sums[0] + sums[1]
            half[1, y] = sums[0] - sums[1]
        pieces += [half[e, y] for e in range(2) for y in range(4)]
    turned = jnp.concatenate(pieces, axis=0).T
    lhs[...] = jnp.zeros(lhs.shape, jnp.float32)
    for e in range(2):
        for l in range(HALF):
            first = jnp.zeros((8, 128), jnp.float32)
            last = jnp.zeros((8, 128), jnp.float32)
            for rt in range(TILES):
                v, p = divmod(rt * HALF + l, 16)
                x = turned[8 * p : 8 * p + 8, :]
                x = roll(x, 32 * (rt % 4) - (64 * v + 32 * e))
                here = (lane >= 32 * (rt % 4)) & (lane < 32 * (rt % 4) + 32)
                if rt < 4:
                    first = jnp.where(here, x, first)
                else:
                    last = jnp.where(here, x, last)
            for s in range(4):
                lhs[s, 16 * e + 2 * l : 16 * e + 2 * l + 2, 0:128] = first[2 * s : 2 * s + 2, :]
                lhs[s, 16 * e + 2 * l : 16 * e + 2 * l + 2, 128:256] = last[2 * s : 2 * s + 2, :]
    slot = lax.axis_index("lon") * 16 + lax.axis_index("y") * 4
    degree = lax.broadcasted_iota(jnp.int32, (16, DEG), 1)
    low = lax.broadcasted_iota(jnp.int32, (8, 128), 0) < 4
    for s in range(4):
        wave = wave_map[slot + s]
        a_hi, a_lo = split(lhs[s][:, 0:160])
        rows = []
        for rt in range(TILES):
            at = slice(40 * s + 8 * rt, 40 * s + 8 * rt + 8)
            rows += [legendre[place, at, :], from_1[at, :], from_2[at, :], from_3[at, :]]
        b_hi, b_lo = split(jnp.concatenate(rows, axis=0))
        sums = dot(a_hi, b_hi) + (dot(a_lo, b_hi) + dot(a_hi, b_lo))
        picked = jnp.where((degree + wave) % 2 == 0, sums[0:16], sums[16:32])
        picked = jnp.where(degree >= wave, picked, 0.0)
        for j in range(10):
            out[s, 8 * j : 8 * j + 8, :] = picked[0:8, 128 * j : 128 * j + 128]
        for j in range(0, 10, 2):
            a = picked[8:16, 128 * j : 128 * j + 128]
            b = picked[8:16, 128 * j + 128 : 128 * j + 256]
            out[s, 80 + 4 * j : 88 + 4 * j, :] = jnp.where(low, a, pltpu.roll(b, 4, 0))


def finish_kernel(helm, parts, out):
    total = parts[0] + parts[1] + (parts[2] + parts[3])
    row = lax.broadcasted_iota(jnp.int32, (8, 128), 0)
    lane = lane_iota()

    def damped(x, first, degree):
        coef = jnp.zeros((8, 128), jnp.float32)
        for i in range(4):
            coef = jnp.where(row // 2 == i, helm[(first + i) % HALF if first + i < HALF else 4 + i % 2], coef)
        return x / (1.0 + coef * (degree * (degree + 1.0)))

    for j in range(10):
        degree = (lane + 128 * j).astype(jnp.float32)
        x = damped(total[8 * j : 8 * j + 8, :], 0, degree)
        for i in range(8):
            l, q = divmod(i, 2)
            out[l, 0, 0, q * DEG + 128 * j : q * DEG + 128 * j + 128] = x[i, :]
    for j in range(0, 10, 2):
        degree = (lane + 128 * j + jnp.where(row < 4, 0, 128)).astype(jnp.float32)
        x = damped(total[80 + 4 * j : 88 + 4 * j, :], 4, degree)
        for i in range(8):
            l, q = divmod(i % 4, 2)
            at = q * DEG + 128 * (j + i // 4)
            out[4 + l, 0, 0, at : at + 128] = x[i, :]


def zonal_table(wave_map):
    col = lax.broadcasted_iota(jnp.int32, (COLS, 128), 0)
    lane = lax.broadcasted_iota(jnp.int32, (COLS, 128), 1)
    phase = (col + lax.axis_index("lon") * COLS) * jnp.repeat(wave_map, 2)[None, :] % LON_TOTAL
    phase = (phase + (lane % 2) * (LON_TOTAL // 4)) % LON_TOTAL
    angle = phase.astype(jnp.float32) * (2.0 * math.pi / LON_TOTAL)
    return jnp.cos(angle) / math.sqrt(LON_TOTAL)


def lon_pairs(odd):
    return [r for i in range(odd, 4, 2) for r in ((i, (i + 1) % 4), ((i + 1) % 4, i))]


def lat_pairs(odd):
    route = []
    for i in range(odd, 15, 2):
        for f in range(8):
            low, high = i * 8 + f, (i + 1) * 8 + f
            route += [(low, high), (high, low)]
    if odd:
        for f in range(8):
            route.append((15 * 8 + f, 15 * 8 + (f ^ 1)))
    return route


def call(kernel, outs, count, scratch=(), smem_first=0, alias={}):
    specs = [smem()] * smem_first + [vmem()] * (count - smem_first)
    return pl.pallas_call(
        kernel,
        out_shape=outs,
        in_specs=specs,
        out_specs=jax.tree.map(lambda _: vmem(), outs),
        scratch_shapes=list(scratch),
        input_output_aliases=alias,
        compiler_params=VM,
    )


def shifted():
    return pltpu.VMEM((12 * TILES, 56, 128), jnp.float32)


def run_inner(*args):
    return call(inner_kernel, f32(LEVELS * 24, 128), 8, (shifted(), pltpu.VMEM((LEVELS * 24, COLS), jnp.float32)))(*args)


def run_outer(*args):
    scratch = (
        shifted(),
        pltpu.VMEM((LEVELS * 16, COLS), jnp.float32),
        pltpu.VMEM((LEVELS * 16, 128), jnp.float32),
        pltpu.VMEM((2, LEVELS, 8, COLS), jnp.float32),
        pltpu.VMEM((2, 2, 8, 128), jnp.float32),
    )
    return call(outer_kernel, f32(32, 16, 128), 11, scratch)(*args)


def stages(field, row_shift, col_shift, row_frac, col_frac, wave_map, legendre, helm_coef):
    grid_args = (field, row_shift, col_shift, row_frac, col_frac)
    lat_e, lat_o, lon_e, lon_o = call(edges_kernel, (f32(80, COLS), f32(80, COLS), f32(ROWS, 128), f32(ROWS, 128)), 1)(field)
    lon_e = lax.ppermute(lon_e, "lon", lon_pairs(0))
    lon_o = lax.ppermute(lon_o, "lon", lon_pairs(1))
    lat_e, lat_o = call(corner_kernel, (f32(80, COLS), f32(80, COLS)), 4, alias={2: 0, 3: 1})(lon_e, lon_o, lat_e, lat_o)
    lat_e = lax.ppermute(lat_e, LATF, lat_pairs(0))
    lat_o = lax.ppermute(lat_o, LATF, lat_pairs(1))
    legendre = legendre.reshape(4, 4 * ROWS, DEG)
    place = lax.axis_index("y")
    arrived_rows = [
        lax.ppermute(lax.dynamic_index_in_dim(legendre, place ^ d, 0, keepdims=False), "y", [(i, i ^ d) for i in range(4)])
        for d in (1, 2, 3)
    ]
    table = zonal_table(wave_map)
    inner = run_inner(*grid_args, lon_e, lon_o, table)
    sent = run_outer(*grid_args, lon_e, lon_o, lat_e, lat_o, table, inner)
    arrived = lax.all_to_all(sent, ("y", "lon", "core"), 0, 0, tiled=True)
    parts = call(legendre_kernel, f32(4, 120, 128), 6, (pltpu.VMEM((4, 32, 256), jnp.float32),), 1)(
        wave_map, arrived, legendre, *arrived_rows
    )
    parts = lax.all_to_all(parts, "zh", 0, 0, tiled=True)
    return call(finish_kernel, f32(HALF, 1, 1, 2 * DEG), 2, (), 1)(helm_coef, parts)


def solution(mesh):
    fine = Mesh(mesh.devices.reshape(4, 4, 4, 4, 2), ("y", "zh", "lon", "zl", "core"))
    fold = ("zl", "core")
    block = P(fold, None, LAT, "lon")
    in_specs = (block, block, block, block, block, P(), P("lon", LAT, None), P(fold))
    return jax.shard_map(stages, mesh=fine, in_specs=in_specs, out_specs=P(fold, "lon", LAT, None), check_vma=False)
```

```python
import math

import jax
import jax.numpy as jnp
from jax import lax
from jax.experimental import pallas as pl
from jax.experimental.pallas import tpu as pltpu
from jax.sharding import Mesh, PartitionSpec as P

LEVELS = 12
HALF = 6
ROWS = 40
COLS = 640
TILES = 5
DEG = 1280
LON_TOTAL = 2560
VM = pltpu.CompilerParams(vmem_limit_bytes=48 * 1024 * 1024)
LAT = ("y", "zh")
LATF = ("y", "zh", "zl", "core")


def lane_iota():
    return lax.broadcasted_iota(jnp.int32, (8, 128), 1)


def roll(x, shift):
    shift %= 128
    return pltpu.roll(x, shift, 1) if shift else x


def vmem():
    return pl.BlockSpec(memory_space=pltpu.VMEM)


def smem():
    return pl.BlockSpec(memory_space=pltpu.SMEM)


def f32(*dims):
    return jax.ShapeDtypeStruct(dims, jnp.float32)


def lat_index():
    return lax.axis_index("y") * 4 + lax.axis_index("zh")


def edges_kernel(field, lon_even, lon_odd):
    lane = lane_iota()
    lon_par = lax.axis_index("lon") % 2
    for rt in range(TILES):
        rows = slice(8 * rt, 8 * rt + 8)
        left = jnp.zeros((8, 128), jnp.float32)
        right = jnp.zeros((8, 128), jnp.float32)
        for l in range(LEVELS):
            here = (lane >= 8 * l) & (lane < 8 * l + 6)
            left = jnp.where(here, roll(field[0, l, rows, 0:128], 8 * l), left)
            right = jnp.where(here, roll(field[0, l, rows, 512:640], 8 * l - 122), right)
        lon_even[rows, :] = jnp.where(lon_par == 0, right, left)
        lon_odd[rows, :] = jnp.where(lon_par == 0, left, right)


def corner_kernel(field, lon_even, lon_odd, _shift, _frac, up, down, mirror):
    for l in range(LEVELS):
        up[5 * l : 5 * l + 5, :] = field[0, l, 35:40, :]
        down[6 * l : 6 * l + 6, :] = field[0, l, 0:6, :]
        for j in range(6):
            mirror[6 * l + j : 6 * l + j + 1, :] = field[0, l, 39 - j : 40 - j, :]
    up[60:72, :] = jnp.zeros((12, COLS), jnp.float32)
    down[72:80, :] = jnp.zeros((8, COLS), jnp.float32)
    mirror[72:80, :] = jnp.zeros((8, COLS), jnp.float32)
    for k, ref in enumerate((lon_even, lon_odd)):
        at = slice(128 * k, 128 * k + 128)
        up[60:65, at] = ref[35:40, :]
        down[72:78, at] = ref[0:6, :]
        for j in range(6):
            mirror[72 + j : 73 + j, at] = ref[39 - j : 40 - j, :]


def cubic(t):
    down = t - 1.0
    two = t - 2.0
    up = t + 1.0
    inner = t * down
    outer = up * two
    return (
        inner * two * (-1.0 / 6.0),
        outer * down * 0.5,
        outer * t * (-0.5),
        up * inner * (1.0 / 6.0),
    )


def put_shifted(sh, row, tiles, lane):
    for t in range(TILES):
        for k in range(12):
            off = k - 5
            x = tiles[t + 1]
            if off > 0:
                x = roll(jnp.where(lane >= off, x, tiles[t + 2]), -off)
            elif off < 0:
                x = roll(jnp.where(lane < 128 + off, x, tiles[t]), -off)
            sh[k * TILES + t, row : row + 8, :] = x


def lon_sides(lon_even, lon_odd, rows, lon_par):
    even = lon_even[rows, :]
    odd = lon_odd[rows, :]
    return jnp.where(lon_par == 0, odd, even), jnp.where(lon_par == 0, even, odd)


def dyn_roll(x, shift):
    return pltpu.roll(x, shift, 1)


def spread(shift, weights, offsets=range(12)):
    placed = {}
    for k in offsets:
        value = None
        for a in range(4):
            if 0 <= k - a < 9:
                value = jnp.where(shift == k - a - 4, weights[a], 0.0 if value is None else value)
        placed[k] = value
    return placed


def line_of(sh, at, t, wc, k):
    acc = None
    for o in range(12):
        got = wc[o] * sh[o * TILES + t, at + k - 5 : at + k + 3, :]
        acc = got if acc is None else acc + got
    return acc


def some_rows(sh, at, t, rs, cs, row_frac, col_frac, offsets):
    wc = spread(cs, cubic(col_frac))
    wr = spread(rs, cubic(row_frac), offsets)
    total = None
    for k in offsets:
        part = wr[k] * line_of(sh, at, t, wc, k)
        total = part if total is None else total + part
    return total


def tile_points(sh, at, t, rs, cs, row_frac, col_frac):
    wc = spread(cs, cubic(col_frac))
    line = [line_of(sh, at, t, wc, k) for k in range(12)]
    wr = cubic(row_frac)
    u = rs + 4
    m = u >= 5
    line = [jnp.where(m, line[k + 5], line[k]) for k in range(7)] + [line[7]]
    u = jnp.where(m, u - 5, u)
    m = u >= 3
    line = [jnp.where(m, line[k + 3], line[k]) for k in range(5)] + [line[5]]
    u = jnp.where(m, u - 3, u)
    m = u >= 2
    line = [jnp.where(m, line[k + 2], line[k]) for k in range(4)] + [line[4]]
    m = u == 1
    line = [jnp.where(m, line[k + 1], line[k]) for k in range(4)]
    total = wr[0] * line[0]
    for a in range(1, 4):
        total = total + wr[a] * line[a]
    return total


def lane_tiles(ref, l, rt):
    if len(ref.shape) == 2:
        x = ref[pl.ds(16 * l + 2 * rt, 8), :]
    else:
        x = ref[0, l, pl.ds(8 * rt, 8), :]
    if x.dtype == jnp.bfloat16:
        x = x.astype(jnp.float32)
    return [x[:, 128 * t : 128 * t + 128] for t in range(TILES)]


def main_rows(win, field, lon_even, lon_odd, l, row_tiles, lon_par, lane):
    for rt in row_tiles:
        left, right = lon_sides(lon_even, lon_odd, slice(8 * rt, 8 * rt + 8), lon_par)
        tiles = [dyn_roll(left, (250 - 8 * l) % 128)] + lane_tiles(field, l, rt) + [dyn_roll(right, (128 - 8 * l) % 128)]
        put_shifted(win, 8 + 8 * rt, tiles, lane)


def split(x):
    hi = x.astype(jnp.bfloat16)
    return hi, (x - hi.astype(jnp.float32)).astype(jnp.bfloat16)


def dot(a, b):
    return jnp.dot(a, b, preferred_element_type=jnp.float32)


def zonal(grid, table):
    hi, lo = split(grid)
    t_hi, t_lo = split(table)
    return dot(hi, t_hi) + (dot(lo, t_hi) + dot(hi, t_lo))


def points_of(l, rt, win, row_shift, col_shift, row_frac, col_frac, put, offsets=None):
    params = [lane_tiles(r, l, rt) for r in (row_shift, col_shift, row_frac, col_frac)]
    for t in range(TILES):
        here = [p[t] for p in params]
        if offsets is None:
            put(t, tile_points(win, 8 + 8 * rt, t, *here))
        else:
            put(t, some_rows(win, 8 + 8 * rt, t, *here, offsets))


def inner_kernel(field, row_shift, col_shift, row_frac, col_frac, lon_even, lon_odd, table, out, partial, edge_shift, win, grid):
    lane = lane_iota()
    lon_par = lax.axis_index("lon") % 2

    def level(l, carry):
        for i, rt in enumerate((0, 4)):
            edge_shift[pl.ds(16 * l + 8 * i, 8), :] = col_shift[0, l, 8 * rt : 8 * rt + 8, :]
        main_rows(win, field, lon_even, lon_odd, l, range(TILES), lon_par, lane)
        for i in range(3):

            def put(w, x, i=i):
                grid[pl.ds(24 * l + 8 * i, 8), 128 * w : 128 * w + 128] = x

            points_of(l, i + 1, win, row_shift, col_shift, row_frac, col_frac, put)
        for i, rt, offsets in ((0, 0, range(5, 12)), (1, 4, range(0, 6))):

            def put_part(w, x, i=i):
                partial[pl.ds(16 * l + 8 * i, 8), 128 * w : 128 * w + 128] = x

            points_of(l, rt, win, row_shift, col_shift, row_frac, col_frac, put_part, offsets)
        return carry

    lax.fori_loop(0, LEVELS, level, 0)
    out[...] = zonal(grid[...], table[...])


def transposed_groups(block, lane):
    group = lane // 8
    for k in (8, 4, 2, 1):
        bit = (group & k) != 0
        new = list(block)
        for i in range(16):
            if not i & k:
                a, b = block[i], block[i + k]
                new[i] = jnp.where(bit, roll(b, 8 * k), a)
                new[i + k] = jnp.where(bit, b, roll(a, -8 * k))
        block = new
    return block


def outer_kernel(
    field,
    row_shift,
    col_shift,
    row_frac,
    col_frac,
    lon_even,
    lon_odd,
    up,
    down,
    mirror,
    table,
    inner,
    partial,
    out,
    win,
    grid,
    zon,
    halo,
    side,
):
    lane = lane_iota()
    lon_par = lax.axis_index("lon") % 2

    for l in range(LEVELS):
        halo[0, l, 0:3, :] = jnp.zeros((3, COLS), jnp.float32)
        halo[0, l, 3:8, :] = up[5 * l : 5 * l + 5, :]
        halo[1, l, 6:8, :] = jnp.zeros((2, COLS), jnp.float32)
    for k in range(2):
        side[0, k, 0:3, :] = jnp.zeros((3, 128), jnp.float32)
        side[0, k, 3:8, :] = up[60:65, 128 * k : 128 * k + 128]
        side[1, k, 6:8, :] = jnp.zeros((2, 128), jnp.float32)

    def place(after):
        for l in range(LEVELS):
            halo[1, l, 0:6, :] = after[6 * l : 6 * l + 6, :]
        for k in range(2):
            side[1, k, 0:6, :] = after[72:78, 128 * k : 128 * k + 128]

    @pl.when(lat_index() < 15)
    def _():
        place(down)

    @pl.when(lat_index() == 15)
    def _():
        place(mirror)

    def level(l, carry):
        main_rows(win, field, lon_even, lon_odd, l, (0, 4), lon_par, lane)
        for k, row in ((0, 0), (1, 48)):
            even = side[k, 0]
            odd = side[k, 1]
            left = jnp.where(lon_par == 0, odd, even)
            right = jnp.where(lon_par == 0, even, odd)
            x = halo[k, l]
            tiles = [x[:, 128 * t : 128 * t + 128] for t in range(TILES)]
            tiles = [dyn_roll(left, (250 - 8 * l) % 128)] + tiles + [dyn_roll(right, (128 - 8 * l) % 128)]
            put_shifted(win, row, tiles, lane)
        for i, rt, offsets in ((0, 0, range(0, 5)), (1, 4, range(6, 12))):

            def put(w, x, i=i):
                at = pl.ds(16 * l + 8 * i, 8)
                lanes = slice(128 * w, 128 * w + 128)
                grid[at, lanes] = partial[at, lanes] + x

            points_of(l, rt, win, row_shift, col_shift, row_frac, col_frac, put, offsets)
        return carry

    lax.fori_loop(0, LEVELS, level, 0)
    zon[...] = zonal(grid[...], table[...])
    for core in range(2):
        for v in range(2):
            block = []
            for p in range(16 * v, 16 * v + 16):
                rt, l = divmod(min(p, 29), HALF)
                l += HALF * core
                if rt in (0, 4):
                    at = 16 * l + (8 if rt else 0)
                    block.append(zon[at : at + 8, :])
                else:
                    at = 24 * l + 8 * (rt - 1)
                    block.append(inner[at : at + 8, :])
            block = transposed_groups(block, lane)
            for d in range(16):
                lon, y = divmod(d, 4)
                out[y * 8 + lon * 2 + core, 8 * v : 8 * v + 8, :] = block[d]


def legendre_kernel(wave_map, arrived, legendre, near, far, other, out, to_1, to_2, to_3, lhs, sums_out, mine, sem):
    lane = lane_iota()
    place = lax.axis_index("y")
    core = lax.axis_index("core")
    fetch = pltpu.make_async_copy(legendre.at[place], mine, sem)
    fetch.start()
    holder = [place, place ^ (1 + core), place ^ (2 - core), place ^ 3]
    pieces = []
    for v in range(2):
        half = {}
        for y in range(4):
            sums = []
            for hemisphere in range(2):
                x = arrived[holder[y] * 8 + hemisphere, 8 * v : 8 * v + 8, :]
                for lon in range(1, 4):
                    x = x + arrived[holder[y] * 8 + lon * 2 + hemisphere, 8 * v : 8 * v + 8, :]
                sums.append(x)
            half[0, y] = sums[0] + sums[1]
            half[1, y] = sums[0] - sums[1]
        pieces += [half[e, y] for e in range(2) for y in range(4)]
    turned = jnp.concatenate(pieces, axis=0).T
    lhs[...] = jnp.zeros(lhs.shape, jnp.float32)
    for e in range(2):
        for l in range(HALF):
            first = jnp.zeros((8, 128), jnp.float32)
            last = jnp.zeros((8, 128), jnp.float32)
            for rt in range(TILES):
                v, p = divmod(rt * HALF + l, 16)
                x = turned[8 * p : 8 * p + 8, :]
                x = roll(x, 32 * (rt % 4) - (64 * v + 32 * e))
                here = (lane >= 32 * (rt % 4)) & (lane < 32 * (rt % 4) + 32)
                if rt < 4:
                    first = jnp.where(here, x, first)
                else:
                    last = jnp.where(here, x, last)
            for s in range(4):
                lhs[s, 16 * e + 2 * l : 16 * e + 2 * l + 2, 0:128] = first[2 * s : 2 * s + 2, :]
                lhs[s, 16 * e + 2 * l : 16 * e + 2 * l + 2, 128:256] = last[2 * s : 2 * s + 2, :]
    slot = lax.axis_index("lon") * 16 + lax.axis_index("y") * 4
    degree = lax.broadcasted_iota(jnp.int32, (16, DEG), 1)
    low = lax.broadcasted_iota(jnp.int32, (8, 128), 0) < 4
    fetch.wait()
    for i in range(4):
        s = 2 * core + i if i < 2 else 2 * (1 - core) + i - 2
        to = s ^ lax.axis_index("zh")
        wave = wave_map[slot + s]
        a_hi, a_lo = split(lhs[s][:, 0:160])
        rows = []
        for rt in range(TILES):
            whole = pl.ds(pl.multiple_of(40 * s + 8 * rt, 8), 8)
            at = 40 * (i % 2) + 8 * rt
            rows += [mine[whole, :], near[whole, :], other[whole, :]]
            rows.append(far[at : at + 8, :] if i < 2 else other[160 + at : 168 + at, :])
        b_hi, b_lo = split(jnp.concatenate(rows, axis=0))
        sums = dot(a_hi, b_hi) + (dot(a_lo, b_hi) + dot(a_hi, b_lo))
        picked = jnp.where((degree + wave) % 2 == 0, sums[0:16], sums[16:32])
        picked = jnp.where(degree >= wave, picked, 0.0)
        for j in range(10):
            sums_out[to, 8 * j : 8 * j + 8, :] = picked[0:8, 128 * j : 128 * j + 128]
        for j in range(0, 10, 2):
            a = picked[8:16, 128 * j : 128 * j + 128]
            b = picked[8:16, 128 * j + 128 : 128 * j + 256]
            sums_out[to, 80 + 4 * j : 88 + 4 * j, :] = jnp.where(low, a, pltpu.roll(b, 4, 0))
    for d, ref in enumerate((out, to_1, to_2, to_3)):
        ref[...] = sums_out[d]


def finish_kernel(helm, own, part_1, part_2, part_3, out):
    total = own[...] + part_1[...] + (part_2[...] + part_3[...])
    row = lax.broadcasted_iota(jnp.int32, (8, 128), 0)
    lane = lane_iota()

    def damped(x, first, degree):
        coef = jnp.zeros((8, 128), jnp.float32)
        for i in range(4):
            coef = jnp.where(row // 2 == i, helm[(first + i) % HALF if first + i < HALF else 4 + i % 2], coef)
        return x / (1.0 + coef * (degree * (degree + 1.0)))

    for j in range(10):
        degree = (lane + 128 * j).astype(jnp.float32)
        x = damped(total[8 * j : 8 * j + 8, :], 0, degree)
        for i in range(8):
            l, q = divmod(i, 2)
            out[l, 0, 0, q * DEG + 128 * j : q * DEG + 128 * j + 128] = x[i, :]
    for j in range(0, 10, 2):
        degree = (lane + 128 * j + jnp.where(row < 4, 0, 128)).astype(jnp.float32)
        x = damped(total[80 + 4 * j : 88 + 4 * j, :], 4, degree)
        for i in range(8):
            l, q = divmod(i % 4, 2)
            at = q * DEG + 128 * (j + i // 4)
            out[4 + l, 0, 0, at : at + 128] = x[i, :]


def zonal_table(wave_map):
    slot = lax.broadcasted_iota(jnp.int32, (64, 128), 0)
    pair = lax.broadcasted_iota(jnp.int32, (64, 128), 1) // 2
    wave = jnp.sum(jnp.where(slot == pair, wave_map[:, None], 0), axis=0)[None, :]

    def angle(col, quarter):
        phase = (col * wave + quarter * (LON_TOTAL // 4)) % LON_TOTAL
        return phase.astype(jnp.float32) * (2.0 * math.pi / LON_TOTAL)

    lane = lax.broadcasted_iota(jnp.int32, (80, 128), 1)
    coarse = angle(lax.axis_index("lon") * COLS + 8 * lax.broadcasted_iota(jnp.int32, (80, 128), 0), lane % 2)
    fine = angle(lax.broadcasted_iota(jnp.int32, (8, 128), 0), 0)
    scale = 1.0 / math.sqrt(LON_TOTAL)
    c, d = jnp.cos(coarse) * scale, jnp.sin(coarse) * scale
    table = c[:, None, :] * jnp.cos(fine)[None] - d[:, None, :] * jnp.sin(fine)[None]
    return table.reshape(COLS, 128)


def lon_pairs(odd):
    return [r for i in range(odd, 4, 2) for r in ((i, (i + 1) % 4), ((i + 1) % 4, i))]


def lat_shift(step):
    return [(i * 8 + f, (i + step) * 8 + f) for i in range(16) for f in range(8) if 0 <= i + step < 16]


def equator():
    return [(15 * 8 + f, 15 * 8 + (f ^ 1)) for f in range(8)]


def call(kernel, outs, count, scratch=(), smem_first=0, whole=None):
    specs = [smem()] * smem_first + [vmem()] * (count - smem_first)
    if whole is not None:
        specs[whole] = pl.BlockSpec(memory_space=pl.ANY)
    return pl.pallas_call(
        kernel,
        out_shape=outs,
        in_specs=specs,
        out_specs=jax.tree.map(lambda _: vmem(), outs),
        scratch_shapes=list(scratch),
        compiler_params=VM,
    )


def shifted():
    return pltpu.VMEM((12 * TILES, 56, 128), jnp.float32)


def run_inner(*args):
    outs = (f32(LEVELS * 24, 128), f32(LEVELS * 16, COLS), jax.ShapeDtypeStruct((LEVELS * 16, COLS), jnp.int32))
    return call(inner_kernel, outs, 8, (shifted(), pltpu.VMEM((LEVELS * 24, COLS), jnp.float32)))(*args)


def run_outer(*args):
    scratch = (
        shifted(),
        pltpu.VMEM((LEVELS * 16, COLS), jnp.float32),
        pltpu.VMEM((LEVELS * 16, 128), jnp.float32),
        pltpu.VMEM((2, LEVELS, 8, COLS), jnp.float32),
        pltpu.VMEM((2, 2, 8, 128), jnp.float32),
    )
    return call(outer_kernel, f32(32, 16, 128), 13, scratch)(*args)


def stages(field, row_shift, col_shift, row_frac, col_frac, wave_map, legendre, helm_coef):
    grid_args = (field, row_shift, col_shift, row_frac, col_frac)
    lon_e, lon_o = call(edges_kernel, (f32(ROWS, 128), f32(ROWS, 128)), 1)(field)
    lon_e = lax.ppermute(lon_e, "lon", lon_pairs(0))
    lon_o = lax.ppermute(lon_o, "lon", lon_pairs(1))
    edge = (f32(72, COLS), f32(80, COLS), f32(80, COLS))
    up, down, mirror = call(corner_kernel, edge, 5)(field, lon_e, lon_o, col_shift, col_frac)
    up = lax.ppermute(up, LATF, lat_shift(1))
    down = lax.ppermute(down, LATF, lat_shift(-1))
    mirror = lax.ppermute(mirror, LATF, equator())
    place = lax.axis_index("y")
    core = lax.axis_index("core")
    by_y = legendre.reshape(4, 4, ROWS, DEG)
    near = lax.dynamic_slice(by_y, (place ^ (1 + core), 0, 0, 0), (1, 4, ROWS, DEG)).reshape(4 * ROWS, DEG)
    far = lax.dynamic_slice(by_y, (place ^ 3, 2 * core, 0, 0), (1, 2, ROWS, DEG)).reshape(2 * ROWS, DEG)
    near = lax.ppermute(near, ("y", "core"), [(2 * i + c, 2 * (i ^ (1 + c)) + c) for i in range(4) for c in range(2)])
    far = lax.ppermute(far, "y", [(i, i ^ 3) for i in range(4)])
    other = lax.ppermute(jnp.concatenate([near, far], axis=0), "core", [(0, 1), (1, 0)])
    legendre = legendre.reshape(4, 4 * ROWS, DEG)
    table = zonal_table(wave_map)
    inner, partial, edge_shift = run_inner(*grid_args, lon_e, lon_o, table)
    sent = run_outer(field, row_shift, edge_shift, row_frac, col_frac, lon_e, lon_o, up, down, mirror, table, inner, partial)
    arrived = lax.all_to_all(sent, ("y", "lon", "core"), 0, 0, tiled=True)
    block = f32(120, 128)
    scratch = (
        pltpu.VMEM((4, 32, 256), jnp.float32),
        pltpu.VMEM((4, 120, 128), jnp.float32),
        pltpu.VMEM((4 * ROWS, DEG), jnp.float32),
        pltpu.SemaphoreType.DMA(()),
    )
    own, *parts = call(legendre_kernel, (block,) * 4, 6, scratch, 1, whole=2)(wave_map, arrived, legendre, near, far, other)
    for d in (2, 1, 3):
        parts[d - 1] = lax.ppermute(parts[d - 1], "zh", [(i, i ^ d) for i in range(4)])
    return call(finish_kernel, f32(HALF, 1, 1, 2 * DEG), 5, (), 1)(helm_coef, own, *parts)


def solution(mesh):
    fine = Mesh(mesh.devices.reshape(4, 4, 4, 4, 2), ("y", "zh", "lon", "zl", "core"))
    fold = ("zl", "core")
    block = P(fold, None, LAT, "lon")
    in_specs = (block, block, block, block, block, P(), P("lon", LAT, None), P(fold))
    return jax.shard_map(stages, mesh=fine, in_specs=in_specs, out_specs=P(fold, "lon", LAT, None), check_vma=False)
```
